32 devices in a mesh: rep: 4 (over x, core), shard: 4 (over z), seq: 2 (over y).
Axes of the slice: x: 2, y: 2, z: 4, core: 2. Of those that a mesh axis runs over, the one named last changes fastest.
Arguments:
- tokens: bfloat16 [16, 1040, 1024], P(('rep', 'shard'), 'seq'), may hold values from -6 to 6
- cotangent: bfloat16 [16, 1040, 1024], P(('rep', 'shard'), 'seq'), may hold values from -6 to 6
- pad_mask: int32 [16, 1040], P(('rep', 'shard'), 'seq'), may hold values from 0 to 1, as said below
- image_mask: int32 [16], P(('rep', 'shard')), may hold values from 0 to 1, as said below
- patch_rows: int32 [16, 1040], P(('rep', 'shard'), 'seq'), may hold values from -1 to 31, as said below
- patch_cols: int32 [16, 1040], P(('rep', 'shard'), 'seq'), may hold values from -1 to 31, as said below
- norm1_gain: float32 [1024], replicated, may hold values from 0.25 to 1.75
- norm1_bias: float32 [1024], replicated, may hold values from -4 to 4
- w_qkv: bfloat16 [1024, 3072], P(('shard', 'seq')), may hold values from -0.1875 to 0.1875
- query_bias: float32 [1024], replicated, may hold values from -6 to 6
- value_bias: float32 [1024], replicated, may hold values from -6 to 6
- attn_gain: float32 [1024], replicated, may hold values from 0.25 to 1.75
- attn_bias: float32 [1024], replicated, may hold values from -4 to 4
- w_proj: bfloat16 [1024, 1024], P(('shard', 'seq')), may hold values from -0.1875 to 0.1875
- proj_bias: float32 [1024], replicated, may hold values from -6 to 6
- norm2_gain: float32 [1024], replicated, may hold values from 0.25 to 1.75
- norm2_bias: float32 [1024], replicated, may hold values from -4 to 4
- w_gate: bfloat16 [1024, 2730], P(('shard', 'seq')), may hold values from -0.1875 to 0.1875
- gate_bias: float32 [2730], replicated, may hold values from -6 to 6
- w_up: bfloat16 [1024, 2730], P(('shard', 'seq')), may hold values from -0.1875 to 0.1875
- up_bias: float32 [2730], replicated, may hold values from -6 to 6
- ffn_gain: float32 [2730], replicated, may hold values from 0.25 to 1.75
- ffn_bias: float32 [2730], replicated, may hold values from -4 to 4
- w_down: bfloat16 [2730, 1024], P(None, ('shard', 'seq')), may hold values from -0.109375 to 0.109375
- down_bias: float32 [1024], replicated, may hold values from -6 to 6
Outputs:
- output: bfloat16 [16, 1040, 1024], P(('rep', 'shard'), 'seq')
- tokens_grad: float32 [16, 1040, 1024], P(('rep', 'shard'), 'seq')
- norm1_gain_grad: float32 [1024], replicated
- norm1_bias_grad: float32 [1024], replicated
- w_qkv_grad: float32 [1024, 3072], P(('shard', 'seq'))
- query_bias_grad: float32 [1024], replicated
- value_bias_grad: float32 [1024], replicated
- attn_gain_grad: float32 [1024], replicated
- attn_bias_grad: float32 [1024], replicated
- w_proj_grad: float32 [1024, 1024], P(('shard', 'seq'))
- proj_bias_grad: float32 [1024], replicated
- norm2_gain_grad: float32 [1024], replicated
- norm2_bias_grad: float32 [1024], replicated
- w_gate_grad: float32 [1024, 2730], P(('shard', 'seq'))
- gate_bias_grad: float32 [2730], replicated
- w_up_grad: float32 [1024, 2730], P(('shard', 'seq'))
- up_bias_grad: float32 [2730], replicated
- ffn_gain_grad: float32 [2730], replicated
- ffn_bias_grad: float32 [2730], replicated
- w_down_grad: float32 [2730, 1024], P(None, ('shard', 'seq'))
- down_bias_grad: float32 [1024], replicated
The draws below stay inside these ranges and needn't reach their ends.
Inputs may be any that keep to these rules, and one draw needn't show every extreme that they name: `pad_mask`: 1 on exactly 1025 slots of each image (its class token and its patches), in an order drawn for each image. `image_mask`: 0 for exactly one image. `patch_rows`: each patch of the 32 x 32 grid stands on one slot of every image; -1 on the class token and on padding. `patch_cols`: the column of the same patch as patch_rows; -1 on the same slots.
All inputs are finite; a program needn't handle non-finite values.
Results may differ from the reference program's by a relative error of at most 0.015.
Values may be sent and summed in bfloat16 or wider, within the bound.
A program may use at most 192 MiB of HBM per device.

```python
import jax
import jax.numpy as jnp
from jax import lax

D = 1024
HEADS = 16
HEAD = 64
FF = 2730
GRID = 32
SLOTS = 1040
IMAGES = 16


def slot_codes(key):
    folded = jax.random.fold_in(key, 17)
    image_keys = jax.random.split(folded, IMAGES)
    return jax.vmap(lambda single: jax.random.permutation(single, SLOTS))(image_keys)


def draw_pad_mask(key, part):
    codes = slot_codes(key)
    return (codes <= GRID * GRID).astype(jnp.int32)


def draw_patch_rows(key, part):
    codes = slot_codes(key)
    return jnp.where(codes < GRID * GRID, codes // GRID, -1).astype(jnp.int32)


def draw_patch_cols(key, part):
    codes = slot_codes(key)
    return jnp.where(codes < GRID * GRID, codes % GRID, -1).astype(jnp.int32)


def draw_image_mask(key, part):
    picked = jax.random.randint(jax.random.fold_in(key, 29), (), 0, IMAGES)
    return (jnp.arange(IMAGES) != picked).astype(jnp.int32)


def block_levels(key, shape, shards, low, largest):
    gain, own = 1.0, jax.random.fold_in(key, 6)
    for axis_at, shards_of in shards:
        heights = jnp.exp(jax.random.uniform(jax.random.fold_in(own, axis_at), (shards_of,), jnp.float32, low / len(shards), largest / len(shards)))
        gain = gain * jnp.repeat(heights, shape[axis_at] // shards_of).reshape([-1 if axis == axis_at else 1 for axis in range(len(shape))])
    return gain


def gaussian(rng, extent, spread, bound, shards=(), held_as=jnp.bfloat16):
    result = jax.random.normal(rng, extent, jnp.float32) * spread
    if len(shards) > 0:
        result = block_levels(rng, extent, shards, -0.22, 0.18) * result
    return jnp.clip(result, min=-bound, max=bound).astype(held_as)


def setup_inputs(seed: int = 0) -> dict:
    splits = jax.random.split(jax.random.key(seed), 26)
    tokens = gaussian(splits[0], (IMAGES, SLOTS, D), 1.0, 6.0, ((0, 16), (1, 2)))
    cotangent = gaussian(splits[1], (IMAGES, SLOTS, D), 1.0, 6.0, ((0, 16), (1, 2)))
    pad_mask = draw_pad_mask(jax.random.fold_in(splits[25], 71), 0)
    image_mask = draw_image_mask(jax.random.fold_in(splits[25], 71), 0)
    patch_rows = draw_patch_rows(jax.random.fold_in(splits[25], 71), 0)
    patch_cols = draw_patch_cols(jax.random.fold_in(splits[25], 71), 0)
    norm1_gain = jnp.clip(1.0 + 0.15 * jax.random.normal(splits[6], (D,), jnp.float32), 0.25, 1.75)
    norm1_bias = gaussian(splits[7], (D,), 0.3, 4.0, (), jnp.float32)
    w_qkv = gaussian(splits[8], (D, 3 * D), D ** -0.5, 0.1875, ((0, 8),))
    query_bias = gaussian(splits[9], (D,), 0.5, 6.0, (), jnp.float32)
    value_bias = gaussian(splits[10], (D,), 0.5, 6.0, (), jnp.float32)
    attn_gain = jnp.clip(1.0 + 0.15 * jax.random.normal(splits[11], (D,), jnp.float32), 0.25, 1.75)
    attn_bias = gaussian(splits[12], (D,), 0.3, 4.0, (), jnp.float32)
    w_proj = gaussian(splits[13], (D, D), D ** -0.5, 0.1875, ((0, 8),))
    proj_bias = gaussian(splits[14], (D,), 0.5, 6.0, (), jnp.float32)
    norm2_gain = jnp.clip(1.0 + 0.15 * jax.random.normal(splits[15], (D,), jnp.float32), 0.25, 1.75)
    norm2_bias = gaussian(splits[16], (D,), 0.3, 4.0, (), jnp.float32)
    w_gate = gaussian(splits[17], (D, FF), D ** -0.5, 0.1875, ((0, 8),))
    gate_bias = gaussian(splits[18], (FF,), 0.5, 6.0, (), jnp.float32)
    w_up = gaussian(splits[19], (D, FF), D ** -0.5, 0.1875, ((0, 8),))
    up_bias = gaussian(splits[20], (FF,), 0.5, 6.0, (), jnp.float32)
    ffn_gain = jnp.clip(1.0 + 0.15 * jax.random.normal(splits[21], (FF,), jnp.float32), 0.25, 1.75)
    ffn_bias = gaussian(splits[22], (FF,), 0.3, 4.0, (), jnp.float32)
    w_down = gaussian(splits[23], (FF, D), FF ** -0.5, 0.109375, ((1, 8),))
    down_bias = gaussian(splits[24], (D,), 0.5, 6.0, (), jnp.float32)
    return dict(tokens=tokens, cotangent=cotangent, pad_mask=pad_mask, image_mask=image_mask, patch_rows=patch_rows, patch_cols=patch_cols, norm1_gain=norm1_gain, norm1_bias=norm1_bias, w_qkv=w_qkv, query_bias=query_bias, value_bias=value_bias, attn_gain=attn_gain, attn_bias=attn_bias, w_proj=w_proj, proj_bias=proj_bias, norm2_gain=norm2_gain, norm2_bias=norm2_bias, w_gate=w_gate, gate_bias=gate_bias, w_up=w_up, up_bias=up_bias, ffn_gain=ffn_gain, ffn_bias=ffn_bias, w_down=w_down, down_bias=down_bias)


norm_epsilon = 1e-06
masked_score = -1e+30
highest = lax.Precision.HIGHEST

@jax.custom_vjp
def low(v):
    return lax.optimization_barrier(v.astype(jnp.bfloat16)).astype(jnp.float32)

@jax.custom_vjp
def low_back(v):
    return v

def low_keep(v):
    return (low(v), None)

def low_pass(kept, grad):
    return (grad,)

def back_keep(v):
    return (v, None)

def back_low(kept, grad):
    return (low(grad),)
low.defvjp(low_keep, low_pass)
low_back.defvjp(back_keep, back_low)

def matmul(left, right):
    return jnp.dot(left, right, precision=highest)

def layer_norm(inputs, norm_gain, norm_bias):
    center = inputs - lax.optimization_barrier(jnp.mean(inputs, -1, keepdims=True))
    variance = lax.optimization_barrier(jnp.mean(center * center, -1, keepdims=True))
    return center * lax.rsqrt(variance + norm_epsilon) * norm_gain + norm_bias

def angle_tables(patch_row, patch_col):
    quarter = HEAD // 4
    frequency = 10000.0 ** (-jnp.arange(quarter).astype(jnp.float32) / quarter)
    places = jnp.stack([patch_row, patch_col], -1).astype(jnp.float32)
    angles = places[:, :, None] * frequency
    rotated = (patch_row >= 0)[:, None, None]
    cosine = jnp.where(rotated, jnp.cos(angles), 1.0)
    sine_table = jnp.where(rotated, jnp.sin(angles), 0.0)
    return (cosine[:, None, :, None, :], sine_table[:, None, :, None, :])

def rotate(vectors, cosine, sine_table):
    row_count = vectors.shape[0]
    shaped = vectors.reshape(row_count, HEADS, 2, 2, HEAD // 4)
    turned = jnp.stack([-shaped[:, :, :, 1], shaped[:, :, :, 0]], 3)
    return (shaped * cosine + turned * sine_table).reshape(row_count, HEADS, HEAD)

def forward(params, inputs, patch_row, patch_col, key_live):
    norm1_gain, norm1_bias, w_qkv, query_bias, value_bias, attn_gain, attn_bias, w_proj, proj_bias, norm2_gain, norm2_bias, w_gate, gate_bias, w_up, up_bias, ffn_gain, ffn_bias, w_down, down_bias = params
    row_count = inputs.shape[0]
    normed = low(layer_norm(inputs, norm1_gain, norm1_bias))
    bias_all = jnp.concatenate([query_bias, jnp.zeros_like(query_bias), value_bias])
    projected = low_back(matmul(normed, w_qkv) + bias_all)
    cosine, sine_table = angle_tables(patch_row, patch_col)
    queries = low(rotate(projected[:, :D].reshape(row_count, HEADS, HEAD), cosine, sine_table))
    key_rows = low(rotate(projected[:, D:2 * D].reshape(row_count, HEADS, HEAD), cosine, sine_table))
    values = low(projected[:, 2 * D:].reshape(row_count, HEADS, HEAD))
    scores = low_back(jnp.einsum('qhe,khe->hqk', queries, key_rows, precision=highest) * HEAD ** (-0.5))
    scores = jnp.where(key_live[None, None, :], scores, masked_score)
    attention = low(jax.nn.softmax(scores, -1))
    context = low_back(jnp.einsum('hqk,khe->qhe', attention, values, precision=highest).reshape(row_count, D))
    normed_attn = low(layer_norm(context, attn_gain, attn_bias))
    middle = inputs + low_back(matmul(normed_attn, w_proj) + proj_bias)
    normed_two = low(layer_norm(middle, norm2_gain, norm2_bias))
    gate_out = low_back(matmul(normed_two, w_gate) + gate_bias)
    up_out = low_back(matmul(normed_two, w_up) + up_bias)
    hidden = jax.nn.silu(gate_out) * up_out
    normed_ffn = low(layer_norm(hidden, ffn_gain, ffn_bias))
    return middle + low_back(matmul(normed_ffn, w_down) + down_bias)

def reference(tokens, cotangent, pad_mask, image_mask, patch_rows, patch_cols, norm1_gain, norm1_bias, w_qkv, query_bias, value_bias, attn_gain, attn_bias, w_proj, proj_bias, norm2_gain, norm2_bias, w_gate, gate_bias, w_up, up_bias, ffn_gain, ffn_bias, w_down, down_bias):
    params = tuple((weight.astype(jnp.float32) for weight in (norm1_gain, norm1_bias, w_qkv, query_bias, value_bias, attn_gain, attn_bias, w_proj, proj_bias, norm2_gain, norm2_bias, w_gate, gate_bias, w_up, up_bias, ffn_gain, ffn_bias, w_down, down_bias)))

    def one_image(totals, pieces):
        image_rows, grad_image, padding, image_alive, patch_row, patch_col = pieces
        key_live = padding > 0
        loss_weight = (padding * image_alive).astype(jnp.float32)

        def forward_one(params_in, inputs):
            return forward(params_in, inputs, patch_row, patch_col, key_live)
        output, pullback = jax.vjp(forward_one, params, image_rows.astype(jnp.float32))
        grads_params, grads_image = pullback(grad_image.astype(jnp.float32) * loss_weight[:, None])
        totals = jax.tree.map(jnp.add, totals, grads_params)
        return (totals, (output.astype(jnp.bfloat16), grads_image))
    zeros_start = jax.tree.map(jnp.zeros_like, params)
    totals, (outputs, input_grads) = lax.scan(one_image, zeros_start, (tokens, cotangent, pad_mask, image_mask, patch_rows, patch_cols))
    return (outputs, input_grads, totals[0], totals[1], totals[2], totals[3], totals[4], totals[5], totals[6], totals[7], totals[8], totals[9], totals[10], totals[11], totals[12], totals[13], totals[14], totals[15], totals[16], totals[17], totals[18])
```

```python
import jax
import jax.numpy as jnp
from jax import lax
from jax.sharding import PartitionSpec as P

HEADS = 16
HEAD = 64
LANES = 128

norm_epsilon = 1e-06
masked_score = -1e30


def product(left, right):
    return jnp.dot(left, right, preferred_element_type=jnp.float32)


def back_product(left, right):
    return lax.dot_general(
        left, right, (((1,), (1,)), ((), ())), preferred_element_type=jnp.float32
    )


def outer_product(left, right):
    return lax.dot_general(
        left, right, (((0,), (0,)), ((), ())), preferred_element_type=jnp.float32
    )


def angle_tables(patch_row, patch_col):
    quarter = HEAD // 4
    frequency = 10000.0 ** (-jnp.arange(quarter).astype(jnp.float32) / quarter)
    places = jnp.stack([patch_row, patch_col], -1).astype(jnp.float32)
    angles = places[:, :, None] * frequency
    rotated = (patch_row >= 0)[:, None, None]
    cosine = jnp.where(rotated, jnp.cos(angles), 1.0)
    sine_table = jnp.where(rotated, jnp.sin(angles), 0.0)
    return (cosine[:, None, :, None, :], sine_table[:, None, :, None, :])


def rotate(vectors, cosine, sine_table):
    row_count = vectors.shape[0]
    shaped = vectors.reshape(row_count, HEADS, 2, 2, HEAD // 4)
    turned = jnp.stack([-shaped[:, :, :, 1], shaped[:, :, :, 0]], 3)
    return (shaped * cosine + turned * sine_table).reshape(row_count, HEADS * HEAD)


class Comm:
    def __init__(self, shape):
        self.rep, self.shard, self.seq = shape["rep"], shape["shard"], shape["seq"]
        assert self.rep == 4 and self.seq == 2
        assert self.shard & (self.shard - 1) == 0
        self.core = lax.axis_index("rep") % 2
        self.x = lax.axis_index("rep") // 2
        self.z = lax.axis_index("shard")
        self.y = lax.axis_index("seq")
        self.bits = self.shard.bit_length() - 1

    def partner(self, array, axis):
        name, size, step = {
            "core": ("rep", self.rep, 1),
            "x": ("rep", self.rep, 2),
            "y": ("seq", self.seq, 1),
        }.get(axis) or ("shard", self.shard, 1 << axis)
        return lax.ppermute(array, name, [(i, i ^ step) for i in range(size)])

    def place(self, axis):
        if axis in ("core", "x", "y"):
            return getattr(self, axis)
        return (self.z >> axis) & 1

    def trade(self, array):
        pairs = []
        for x in range(2):
            for c in range(2):
                for y in range(2):
                    pairs.append(((x * 2 + c) * 2 + y, (x * 2 + y) * 2 + c))
        return lax.ppermute(array, ("rep", "seq"), pairs)

    def merge(self, held, came, axis):
        slot = lax.broadcasted_iota(jnp.int32, (1, 2) + (1,) * (held.ndim - 1), 1)
        return jnp.where(slot == self.place(axis), held[:, None], came[:, None])

    def gather(self, piece, last):
        rows, cols = piece.shape
        held = piece[None]
        for bit in reversed(range(self.bits)):
            merged = self.merge(held, self.partner(held, bit), bit)
            held = merged.reshape(-1, rows, cols)
        if last == "x":
            held = self.merge(held, self.partner(held, "y"), "y").reshape(-1, rows, cols)
            held = self.merge(held, self.partner(held, "x"), "x").reshape(-1, rows, cols)
        else:
            held = self.merge(held, self.partner(held, "x"), "x").reshape(-1, 2 * rows, cols)
            held = self.merge(held, self.partner(held, "y"), "y")
        return held.reshape(-1, cols)

    def halve(self, array, axis, dim):
        mine = lax.dynamic_index_in_dim(array, self.place(axis), dim, keepdims=False)
        other = lax.dynamic_index_in_dim(array, 1 - self.place(axis), dim, keepdims=False)
        came = self.partner(other, axis)
        return (mine.astype(jnp.float32) + came.astype(jnp.float32)).astype(array.dtype)

    def scatter(self, mine, other, first):
        came = self.partner(other, "core")
        held = (mine.astype(jnp.float32) + came.astype(jnp.float32)).astype(jnp.bfloat16)
        cols = held.shape[1]
        rows = held.shape[0] // (self.shard * 4)
        held = held.reshape(self.shard, 2, 2, rows, cols)
        if first == "x":
            held = self.halve(held, "x", 2)
            held = self.halve(held, "y", 1)
        else:
            held = self.halve(held, "y", 1)
            held = self.halve(held, "x", 1)
        for bit in range(self.bits):
            held = self.halve(held.reshape(-1, 2, rows, cols), bit, 1)
        held = self.merge(held.reshape(1, rows, cols), self.partner(held.reshape(1, rows, cols), "x"), "x")
        held = held.reshape(2 * rows, cols)
        return held, self.partner(held, "core")

    def total(self, vector):
        for axis in ["core", "x", "y"] + list(range(self.bits)):
            vector = vector + self.partner(vector, axis)
        return vector

    def relative(self, panels):
        return jnp.where(self.core == 0, panels, panels[..., ::-1, :])


def on_device(shape, tokens, cotangent, pad_mask, image_mask, patch_rows, patch_cols,
              norm1_gain, norm1_bias, w_qkv, query_bias, value_bias, attn_gain, attn_bias,
              w_proj, proj_bias, norm2_gain, norm2_bias, w_gate, gate_bias, w_up, up_bias,
              ffn_gain, ffn_bias, w_down, down_bias):
    comm = Comm(shape)
    images, slot_count, width = tokens.shape
    assert images == 1
    half = width // 2
    rows = slot_count
    hidden_width = w_gate.shape[1]
    panel = -(-hidden_width // (2 * LANES)) * LANES
    score_scale = HEAD ** (-0.5)
    block = w_qkv.shape[0]

    def ff_panels(array):
        pad = [(0, 0)] * (array.ndim - 1) + [(0, 2 * panel - hidden_width)]
        return jnp.pad(array, pad).reshape(array.shape[:-1] + (2, panel))

    def own(array):
        mine = lax.dynamic_index_in_dim(array, comm.core, 1, keepdims=False)
        return lax.dynamic_slice_in_dim(mine, comm.x * (block // 2), block // 2, 0)

    swapped_tokens = comm.trade(tokens.reshape(rows, width))
    packed = jnp.concatenate(
        [pad_mask, patch_rows, patch_cols, jnp.broadcast_to(image_mask[:, None], pad_mask.shape)], 0
    )
    packed = comm.trade(packed)
    live = packed[0]
    live_other = comm.partner(packed[:1], "core")[0]
    alive = packed[3]

    qkv = w_qkv.reshape(block, 3, 2, half)
    value_cut = half // 2
    piece_a = own(jnp.concatenate([qkv[:, 0], qkv[:, 2, :, :value_cut]], -1))
    piece_b = own(jnp.concatenate([qkv[:, 1], qkv[:, 2, :, value_cut:]], -1))
    qv_mine = comm.gather(piece_a, "x")
    kv_mine = comm.gather(piece_b, "y")
    qv_other = comm.partner(qv_mine, "core")
    kv_other = comm.partner(kv_mine, "core")
    proj_panels = w_proj.reshape(block, 2, half)
    gate_piece = own(jnp.concatenate([ff_panels(w_gate), proj_panels], -1))
    gate_mine = comm.gather(gate_piece, "x")
    gate_other = comm.partner(gate_mine, "core")
    up_mine = comm.gather(own(ff_panels(w_up)), "y")
    up_other = comm.partner(up_mine, "core")
    down_mine = comm.gather(own(ff_panels(w_down.T)), "x")
    down_other = comm.partner(down_mine, "core")
    proj_mine, proj_other = gate_mine[:, panel:], gate_other[:, panel:]
    gate_mine, gate_other = gate_mine[:, :panel], gate_other[:, :panel]
    w_proj_all = jnp.where(
        comm.core == 0,
        jnp.concatenate([proj_mine, proj_other], 1),
        jnp.concatenate([proj_other, proj_mine], 1),
    )

    def by_core(vector):
        return comm.relative(vector.reshape(2, -1)).reshape(-1)

    def by_ff(vector):
        return comm.relative(ff_panels(vector)).reshape(-1)

    def from_ff(vector):
        return comm.relative(vector.reshape(2, panel)).reshape(-1)[:hidden_width]

    column = lax.broadcasted_iota(jnp.int32, (2, panel), 0) * panel + lax.broadcasted_iota(
        jnp.int32, (2, panel), 1
    )
    ff_live = comm.relative((column < hidden_width).astype(jnp.float32)).reshape(-1)

    def norm_forward(inputs, gain, bias, count=None, real=None):
        count = count or inputs.shape[-1]
        center = inputs - jnp.sum(inputs, -1, keepdims=True) / count
        if real is not None:
            center = center * real
        inverse = lax.rsqrt(jnp.sum(center * center, -1, keepdims=True) / count + norm_epsilon)
        normal = center * inverse
        return (normal * gain + bias, normal, inverse)

    def norm_backward(grad_out, normal, inverse, gain, count=None):
        count = count or normal.shape[-1]
        scaled = grad_out * gain
        adjusted = (
            scaled
            - jnp.sum(scaled, -1, keepdims=True) / count
            - normal * (jnp.sum(scaled * normal, -1, keepdims=True) / count)
        )
        return (adjusted * inverse, jnp.sum(grad_out * normal, 0), jnp.sum(grad_out, 0))

    inputs = swapped_tokens.astype(jnp.float32)
    normed_one, normal_one, inverse_one = norm_forward(inputs, norm1_gain, norm1_bias)
    normed_one = normed_one.astype(jnp.bfloat16)
    query_bias_rel, value_bias_rel = by_core(query_bias), by_core(value_bias)
    qv_m, kv_m = product(normed_one, qv_mine), product(normed_one, kv_mine)
    qv_o, kv_o = product(normed_one, qv_other), product(normed_one, kv_other)
    cosine, sine_table = angle_tables(packed[1], packed[2])
    queries = rotate(
        jnp.concatenate([qv_m[:, :half], qv_o[:, :half]], 1) + query_bias_rel, cosine, sine_table
    ).astype(jnp.bfloat16)
    key_rows = rotate(
        jnp.concatenate([kv_m[:, :half], kv_o[:, :half]], 1), cosine, sine_table
    ).astype(jnp.bfloat16)
    values = (
        jnp.concatenate([qv_m[:, half:], kv_m[:, half:], qv_o[:, half:], kv_o[:, half:]], 1)
        + value_bias_rel
    ).astype(jnp.bfloat16)

    def turn(array):
        return jnp.concatenate([array[:, half:], array[:, :half]], 1)

    keys_all = jnp.concatenate([key_rows, turn(comm.partner(key_rows, "core"))], 0)
    values_all = jnp.concatenate([values, turn(comm.partner(values, "core"))], 0)
    live_all = jnp.concatenate([live, live_other], 0)

    key_open = (live_all > 0)[None, :]

    def heads_of(array):
        return array.reshape(array.shape[0], HEADS, HEAD).transpose(1, 0, 2)

    def flat_of(array):
        return array.transpose(1, 0, 2).reshape(array.shape[1], width)

    query_heads, key_heads, value_heads = heads_of(queries), heads_of(keys_all), heads_of(values_all)

    def attend(pieces):
        query_head, key_head, value_head = pieces
        scores = back_product(query_head, key_head) * score_scale
        scores = jnp.where(key_open, scores, masked_score)
        largest = jnp.max(scores, -1, keepdims=True)
        exponent = jnp.exp(scores - largest)
        denominator = jnp.sum(exponent, -1, keepdims=True)
        attention = (exponent / denominator).astype(jnp.bfloat16)
        return (product(attention, value_head), (largest + jnp.log(denominator))[..., 0])

    context_heads, log_totals = lax.map(attend, (query_heads, key_heads, value_heads))
    context = flat_of(context_heads)
    normed_attn, normal_attn, inverse_attn = norm_forward(context, by_core(attn_gain), by_core(attn_bias))

    def swap_halves(array):
        return jnp.where(comm.core == 0, array, turn(array))

    normed_attn = swap_halves(normed_attn.astype(jnp.bfloat16))
    middle = inputs + product(normed_attn, w_proj_all) + proj_bias
    normed_two, normal_two, inverse_two = norm_forward(middle, norm2_gain, norm2_bias)
    normed_two = normed_two.astype(jnp.bfloat16)
    gate_out = jnp.concatenate([product(normed_two, gate_mine), product(normed_two, gate_other)], 1)
    gate_out = gate_out + by_ff(gate_bias)
    up_out = jnp.concatenate([product(normed_two, up_mine), product(normed_two, up_other)], 1)
    up_out = up_out + by_ff(up_bias)
    sigmoid = jax.nn.sigmoid(gate_out)
    activated = gate_out * sigmoid
    hidden = activated * up_out
    gain_ffn = by_ff(ffn_gain)
    normed_ffn, normal_ffn, inverse_ffn = norm_forward(
        hidden, gain_ffn, by_ff(ffn_bias), hidden_width, ff_live
    )
    normed_ffn = normed_ffn.astype(jnp.bfloat16)
    result = (
        middle
        + back_product(normed_ffn[:, :panel], down_mine)
        + back_product(normed_ffn[:, panel:], down_other)
        + down_bias
    )
    output = comm.trade(result.astype(jnp.bfloat16))

    loss_weight = (live * alive).astype(jnp.float32)
    grad_out = comm.trade(cotangent.reshape(rows, width)).astype(jnp.float32) * loss_weight[:, None]
    grad_down = grad_out.astype(jnp.bfloat16)
    down_bias_grad = jnp.sum(grad_down.astype(jnp.float32), 0)

    def low_outer(left, right):
        return outer_product(left, right).astype(jnp.bfloat16)

    owned_down = comm.scatter(
        low_outer(grad_down, normed_ffn[:, :panel]), low_outer(grad_down, normed_ffn[:, panel:]), "x"
    )
    grad_ffn = jnp.concatenate([product(grad_down, down_mine), product(grad_down, down_other)], 1)
    grad_hidden, ffn_gain_grad, ffn_bias_grad = norm_backward(
        grad_ffn, normal_ffn, inverse_ffn, gain_ffn, hidden_width
    )
    grad_gate = (grad_hidden * up_out * sigmoid * (1.0 + gate_out * (1.0 - sigmoid))).astype(
        jnp.bfloat16
    )
    grad_up = (grad_hidden * activated).astype(jnp.bfloat16)
    gate_bias_grad = jnp.sum(grad_gate.astype(jnp.float32), 0)
    up_bias_grad = jnp.sum(grad_up.astype(jnp.float32), 0)
    owned_gate = comm.scatter(
        low_outer(normed_two, grad_gate[:, :panel]), low_outer(normed_two, grad_gate[:, panel:]), "y"
    )
    owned_up = comm.scatter(
        low_outer(normed_two, grad_up[:, :panel]), low_outer(normed_two, grad_up[:, panel:]), "x"
    )
    grad_normed_two = (
        back_product(grad_gate[:, :panel], gate_mine)
        + back_product(grad_gate[:, panel:], gate_other)
        + back_product(grad_up[:, :panel], up_mine)
        + back_product(grad_up[:, panel:], up_other)
    )
    grad_part_two, norm2_gain_grad, norm2_bias_grad = norm_backward(
        grad_normed_two, normal_two, inverse_two, norm2_gain
    )
    grad_middle = grad_out + grad_part_two
    grad_proj = grad_middle.astype(jnp.bfloat16)
    proj_bias_grad = jnp.sum(grad_proj.astype(jnp.float32), 0)
    grad_proj_rel = swap_halves(grad_proj)
    owned_proj = comm.scatter(
        low_outer(normed_attn, grad_proj_rel[:, :half]),
        low_outer(normed_attn, grad_proj_rel[:, half:]),
        "y",
    )
    grad_context, attn_gain_grad, attn_bias_grad = norm_backward(
        swap_halves(back_product(grad_proj, w_proj_all)), normal_attn, inverse_attn, by_core(attn_gain)
    )
    grad_context_heads = heads_of(grad_context.astype(jnp.bfloat16))

    def attend_back(pieces):
        query_head, key_head, value_head, log_total, grad_head = pieces
        scores = back_product(query_head, key_head) * score_scale
        scores = jnp.where(key_open, scores, masked_score)
        attention = jnp.exp(scores - log_total[..., None])
        attention_low = attention.astype(jnp.bfloat16)
        grad_value = outer_product(attention_low, grad_head)
        grad_attention = back_product(grad_head, value_head)
        row_dot = jnp.sum(grad_attention * attention, -1, keepdims=True)
        grad_scores = (attention * (grad_attention - row_dot)).astype(jnp.bfloat16)
        grad_query = product(grad_scores, key_head) * score_scale
        grad_key = outer_product(grad_scores, query_head) * score_scale
        return (grad_query, grad_key, grad_value)

    grad_query_heads, grad_key_heads, grad_value_heads = lax.map(
        attend_back, (query_heads, key_heads, value_heads, log_totals, grad_context_heads)
    )
    grad_keys_all = flat_of(grad_key_heads)
    grad_values_all = flat_of(grad_value_heads)

    def fold(array):
        came = comm.partner(turn(array[rows:].astype(jnp.bfloat16)), "core")
        return array[:rows] + came.astype(jnp.float32)

    grad_query_flat = rotate(flat_of(grad_query_heads), cosine, -sine_table).astype(jnp.bfloat16)
    grad_key_flat = rotate(fold(grad_keys_all), cosine, -sine_table).astype(jnp.bfloat16)
    grad_value_flat = fold(grad_values_all).astype(jnp.bfloat16)
    query_bias_grad = jnp.sum(grad_query_flat.astype(jnp.float32), 0)
    value_bias_grad = jnp.sum(grad_value_flat.astype(jnp.float32), 0)

    def mixed(main, side):
        return [
            jnp.concatenate(
                [main[:, p * half : (p + 1) * half], grad_value_flat[:, p * half + side : p * half + side + value_cut]], 1
            )
            for p in (0, 1)
        ]

    grad_qv = mixed(grad_query_flat, 0)
    grad_kv = mixed(grad_key_flat, value_cut)
    owned_qv = comm.scatter(low_outer(normed_one, grad_qv[0]), low_outer(normed_one, grad_qv[1]), "x")
    owned_kv = comm.scatter(low_outer(normed_one, grad_kv[0]), low_outer(normed_one, grad_kv[1]), "y")
    grad_normed_one = (
        back_product(grad_qv[0], qv_mine)
        + back_product(grad_qv[1], qv_other)
        + back_product(grad_kv[0], kv_mine)
        + back_product(grad_kv[1], kv_other)
    )
    grad_part_one, norm1_gain_grad, norm1_bias_grad = norm_backward(
        grad_normed_one, normal_one, inverse_one, norm1_gain
    )
    tokens_grad = comm.trade((grad_middle + grad_part_one).astype(jnp.bfloat16)).astype(jnp.float32)

    early = [
        by_core(attn_gain_grad), by_core(attn_bias_grad), proj_bias_grad, norm2_gain_grad,
        norm2_bias_grad, from_ff(gate_bias_grad), from_ff(up_bias_grad), from_ff(ffn_gain_grad),
        from_ff(ffn_bias_grad), down_bias_grad,
    ]
    late = [norm1_gain_grad, norm1_bias_grad, by_core(query_bias_grad), by_core(value_bias_grad)]

    def totals(vectors):
        sizes = [vector.shape[0] for vector in vectors]
        flat = jnp.concatenate(vectors)
        length = -(-flat.shape[0] // 1024) * 1024
        flat = jnp.pad(flat, (0, length - flat.shape[0])).reshape(-1, LANES)
        flat = comm.total(flat).reshape(-1)
        parts, start = [], 0
        for size in sizes:
            parts.append(flat[start : start + size])
            start += size
        return parts

    early, late = totals(early), totals(late)

    def both(pair):
        return jnp.where(
            comm.core == 0, jnp.stack(pair, 1), jnp.stack(pair[::-1], 1)
        ).astype(jnp.float32)

    def from_panels(pair):
        return both(pair).reshape(block, 2 * panel)[:, :hidden_width]

    qv_owned, kv_owned = both(owned_qv), both(owned_kv)
    w_qkv_grad = jnp.concatenate(
        [
            qv_owned[:, :, :half].reshape(block, width),
            kv_owned[:, :, :half].reshape(block, width),
            jnp.concatenate([qv_owned[:, :, half:], kv_owned[:, :, half:]], -1).reshape(block, width),
        ],
        1,
    )
    shape_out = (images, slot_count, width)
    return (
        output.reshape(shape_out),
        tokens_grad.reshape(shape_out),
        late[0],
        late[1],
        w_qkv_grad,
        late[2],
        late[3],
        early[0],
        early[1],
        both(owned_proj).reshape(block, width),
        early[2],
        early[3],
        early[4],
        from_panels(owned_gate),
        early[5],
        from_panels(owned_up),
        early[6],
        early[7],
        early[8],
        from_panels(owned_down).T,
        early[9],
    )


def solution(mesh):
    data, rows, cols, copied = (
        P(("rep", "shard"), "seq", None),
        P(("shard", "seq"), None),
        P(None, ("shard", "seq")),
        P(),
    )
    slots = P(("rep", "shard"), "seq")
    placed = (
        data, data, slots, P(("rep", "shard")), slots, slots, copied, copied, rows, copied, copied,
        copied, copied, rows, copied, copied, copied, rows, copied, rows, copied, copied, copied,
        cols, copied,
    )
    shape = dict(mesh.shape)

    def whole(*arrays):
        return on_device(shape, *arrays)

    return jax.shard_map(
        whole,
        mesh=mesh,
        in_specs=placed,
        out_specs=(
            data, data, copied, copied, rows, copied, copied, copied, copied, rows, copied, copied,
            copied, rows, copied, rows, copied, copied, copied, cols, copied,
        ),
        check_vma=False,
    )
```

```python
import functools

import jax
import jax.numpy as jnp
from jax import lax
from jax.experimental import pallas as pl
from jax.experimental.pallas import tpu as pltpu
from jax.sharding import PartitionSpec as P

HEADS = 16
HEAD = 64
LANES = 128

norm_epsilon = 1e-06
masked_score = -1e30


def product(left, right):
    return jnp.dot(left, right, preferred_element_type=jnp.float32)


def back_product(left, right):
    return lax.dot_general(
        left, right, (((1,), (1,)), ((), ())), preferred_element_type=jnp.float32
    )


def outer_product(left, right):
    return lax.dot_general(
        left, right, (((0,), (0,)), ((), ())), preferred_element_type=jnp.float32
    )


def angle_tables(patch_row, patch_col):
    quarter = HEAD // 4
    lane = jnp.arange(LANES)
    frequency = 10000.0 ** (-(lane % quarter).astype(jnp.float32) / quarter)
    place = jnp.where((lane // (HEAD // 2)) % 2 == 0, patch_row[:, None], patch_col[:, None])
    angles = place.astype(jnp.float32) * frequency
    rotated = (patch_row >= 0)[:, None]
    return (jnp.where(rotated, jnp.cos(angles), 1.0), jnp.where(rotated, jnp.sin(angles), 0.0))


def parts_of(column):
    high = column.astype(jnp.bfloat16).astype(jnp.float32)
    rest = column - high
    middle = rest.astype(jnp.bfloat16).astype(jnp.float32)
    return (high, middle, rest - middle)


def set_lanes(array, lane, first, columns):
    for step, column in enumerate(columns):
        array = jnp.where(lane == first + step, column, array)
    return array


def lane_of(rows, lanes=LANES):
    return lax.broadcasted_iota(jnp.int32, (rows, lanes), 1)


def turn_lanes(array, cosine, sine, back):
    lanes = array.shape[1]
    lane = lane_of(*array.shape)
    ahead, behind = pltpu.roll(array, lanes - 16, 1), pltpu.roll(array, 16, 1)
    first = (lane // 16) % 2 == 0
    turned = jnp.where(first, ahead, -behind) if back else jnp.where(first, -ahead, behind)
    return array * cosine + turned * sine


def project_kernel(x_ref, a_ref, b_ref, bias_ref, cos_ref, sin_ref, q_ref, kv_ref):
    step = pl.program_id(0)

    def times(w_ref):
        return jnp.dot(x_ref[...], w_ref[...], preferred_element_type=jnp.float32) + bias_ref[0]

    def turned(w_ref):
        cosine = jnp.concatenate([cos_ref[...]] * 2, 1)
        sine = jnp.concatenate([sin_ref[...]] * 2, 1)
        return turn_lanes(times(w_ref), cosine, sine, False).astype(jnp.bfloat16)

    @pl.when(step < 2)
    def _():
        q_ref[...] = turned(a_ref)

    @pl.when((step >= 2) & (step < 4))
    def _():
        kv_ref[...] = turned(b_ref)

    @pl.when(step == 4)
    def _():
        kv_ref[...] = times(a_ref).astype(jnp.bfloat16)

    @pl.when(step == 5)
    def _():
        kv_ref[...] = times(b_ref).astype(jnp.bfloat16)


def project(x, weights_a, weights_b, bias, cosine, sine):
    rows, width = x.shape
    cut = weights_a.shape[1] // 3
    whole = lambda j: (0, 0)
    return pl.pallas_call(
        project_kernel,
        grid=(6,),
        in_specs=[
            pl.BlockSpec((rows, width), whole),
            pl.BlockSpec((width, cut), lambda j: (0, jnp.where(j < 1, 0, jnp.where(j < 4, 1, 2)))),
            pl.BlockSpec((width, cut), lambda j: (0, jnp.where(j < 3, 0, jnp.where(j < 5, 1, 2)))),
            pl.BlockSpec((1, 1, cut), lambda j: (j, 0, 0)),
            pl.BlockSpec((rows, LANES), whole),
            pl.BlockSpec((rows, LANES), whole),
        ],
        out_specs=[
            pl.BlockSpec((rows, cut), lambda j: (0, jnp.minimum(j, 1))),
            pl.BlockSpec((rows, cut), lambda j: (0, jnp.maximum(j - 2, 0))),
        ],
        out_shape=[
            jax.ShapeDtypeStruct((rows, 2 * cut), jnp.bfloat16),
            jax.ShapeDtypeStruct((rows, 4 * cut), jnp.bfloat16),
        ],
        name="project",
        cost_estimate=pl.CostEstimate(
            flops=12 * rows * width * cut, transcendentals=0, bytes_accessed=12 * width * cut + 2 * rows * (width + 6 * cut)
        ),
    )(x, weights_a, weights_b, bias.reshape(6, 1, cut), cosine, sine)


def both_rows(near_ref, far_ref):
    return jnp.concatenate([near_ref[...].astype(jnp.float32), far_ref[...].astype(jnp.float32)], 0)


def attend_kernel(q_ref, k_ref, k_far, v_ref, v_far, bias_ref, out_ref, log_ref):
    pair = pl.program_id(0)
    rows = q_ref.shape[0]
    lane, key_lane = lane_of(rows), lane_of(bias_ref.shape[0])
    query = q_ref[...].astype(jnp.float32) * HEAD ** (-0.5)
    key = both_rows(k_ref, k_far)
    value = both_rows(v_ref, v_far).astype(jnp.bfloat16)

    @pl.when(pair == 0)
    def _():
        log_ref[...] = jnp.zeros_like(log_ref)

    out_ref[...] = jnp.zeros_like(out_ref)
    for head in (0, 1):
        spare = HEAD * (1 - head)
        own = (lane // HEAD) == head
        query_one = set_lanes(jnp.where(own, query, 0.0), lane, spare, (1.0,)).astype(jnp.bfloat16)
        key_one = set_lanes(key, key_lane, spare, (bias_ref[...],)).astype(jnp.bfloat16)
        scores = back_product(query_one, key_one)
        largest = jnp.max(scores, -1, keepdims=True)
        exponent = jnp.exp(scores - largest)
        total = jnp.sum(exponent, -1, keepdims=True)
        context = product(exponent.astype(jnp.bfloat16), value) / total
        out_ref[...] = jnp.where(own, context, out_ref[...])
        log_ref[...] = jnp.where(lane == 2 * pair + head, largest + jnp.log(total), log_ref[...])


def attend(q, near, far, bias):
    rows, cols = q.shape
    pairs = cols // LANES
    keys = 2 * rows
    step = lambda p: (0, p)
    later = lambda p: (0, pairs + p)
    whole = lambda p: (0, 0)
    size = rows * keys * 2 * pairs
    one = (rows, LANES)
    return pl.pallas_call(
        attend_kernel,
        grid=(pairs,),
        in_specs=[
            pl.BlockSpec(one, step), pl.BlockSpec(one, step), pl.BlockSpec(one, step),
            pl.BlockSpec(one, later), pl.BlockSpec(one, later), pl.BlockSpec((keys, 1), whole),
        ],
        out_specs=[pl.BlockSpec(one, step), pl.BlockSpec(one, whole)],
        out_shape=[
            jax.ShapeDtypeStruct((rows, cols), jnp.float32),
            jax.ShapeDtypeStruct((rows, LANES), jnp.float32),
        ],
        name="attend",
        cost_estimate=pl.CostEstimate(
            flops=4 * size * 256, transcendentals=size, bytes_accessed=rows * cols * 14
        ),
    )(q, near, far, near, far, bias)


def attend_back_kernel(first, q_ref, k_ref, k_far, v_ref, v_far, bias_ref, ctx_ref, grad_ref, log_ref,
                       cos_ref, sin_ref, gq_ref, near_ref, far_ref, sq, sk, sv):
    pair = pl.program_id(0) + first
    rows, keys = q_ref.shape[0], bias_ref.shape[0]
    lane, key_lane = lane_of(rows), lane_of(keys)
    scale = HEAD ** (-0.5)
    grad = grad_ref[...].astype(jnp.float32)
    key, value = both_rows(k_ref, k_far), both_rows(v_ref, v_far)
    key_low = key.astype(jnp.bfloat16)
    for head in (0, 1):
        spare = HEAD * (1 - head)
        own = (lane // HEAD) == head
        own_key = (key_lane // HEAD) == head
        log_total = jnp.sum(jnp.where(lane == 2 * pair + head, log_ref[...], 0.0), -1, keepdims=True)
        row_dot = jnp.sum(jnp.where(own, grad * ctx_ref[...], 0.0), -1, keepdims=True)
        query_one = set_lanes(
            jnp.where(own, q_ref[...].astype(jnp.float32) * scale, 0.0),
            lane, spare, (1.0,) + parts_of(-log_total),
        ).astype(jnp.bfloat16)
        key_one = set_lanes(key, key_lane, spare, (bias_ref[...], 1.0, 1.0, 1.0)).astype(jnp.bfloat16)
        attention = jnp.exp(back_product(key_one, query_one))
        grad_one = set_lanes(
            jnp.where(own, grad, 0.0), lane, spare, parts_of(-row_dot)
        ).astype(jnp.bfloat16)
        value_one = set_lanes(value, key_lane, spare, (1.0, 1.0, 1.0)).astype(jnp.bfloat16)
        grad_scores = (attention * back_product(value_one, grad_one)).astype(jnp.bfloat16)
        grad_value = product(attention.astype(jnp.bfloat16), grad_ref[...])
        grad_key = product(grad_scores, q_ref[...])
        grad_query = outer_product(grad_scores, key_low)
        sv[...] = jnp.where(own_key, grad_value, sv[...])
        sk[...] = jnp.where(own_key, grad_key, sk[...])
        sq[...] = jnp.where(own, grad_query, sq[...])

    gq_ref[...] = turn_lanes(sq[...] * scale, cos_ref[:rows], sin_ref[:rows], True).astype(jnp.bfloat16)
    grad_key = turn_lanes(sk[...] * scale, cos_ref[...], sin_ref[...], True)
    near_ref[0] = grad_key[:rows].astype(jnp.bfloat16)
    far_ref[0] = grad_key[rows:].astype(jnp.bfloat16)
    near_ref[1] = sv[:rows].astype(jnp.bfloat16)
    far_ref[1] = sv[rows:].astype(jnp.bfloat16)


def attend_back(q, near, far, bias, context, grad, logs, cosine, sine, first, pairs, grad_first):
    rows, cols = q.shape
    keys = 2 * rows
    all_pairs = cols // LANES
    step = lambda p: (0, first + p)
    later = lambda p: (0, all_pairs + first + p)
    whole = lambda p: (0, 0)
    size = rows * keys * 2 * pairs
    one = (rows, LANES)
    sides = pl.BlockSpec((2, rows, LANES), lambda p: (0, 0, p))
    return pl.pallas_call(
        functools.partial(attend_back_kernel, first),
        grid=(pairs,),
        in_specs=[
            pl.BlockSpec(one, step), pl.BlockSpec(one, step), pl.BlockSpec(one, step),
            pl.BlockSpec(one, later), pl.BlockSpec(one, later), pl.BlockSpec((keys, 1), whole),
            pl.BlockSpec(one, step), pl.BlockSpec(one, lambda p: (0, grad_first + p)),
            pl.BlockSpec(one, whole), pl.BlockSpec((keys, LANES), whole), pl.BlockSpec((keys, LANES), whole),
        ],
        out_specs=[pl.BlockSpec(one, lambda p: (0, p)), sides, sides],
        out_shape=[
            jax.ShapeDtypeStruct((rows, LANES * pairs), jnp.bfloat16),
            jax.ShapeDtypeStruct((2, rows, LANES * pairs), jnp.bfloat16),
            jax.ShapeDtypeStruct((2, rows, LANES * pairs), jnp.bfloat16),
        ],
        scratch_shapes=[
            pltpu.VMEM((rows, LANES), jnp.float32),
            pltpu.VMEM((keys, LANES), jnp.float32),
            pltpu.VMEM((keys, LANES), jnp.float32),
        ],
        name="attend_back",
        cost_estimate=pl.CostEstimate(
            flops=10 * size * 256, transcendentals=size, bytes_accessed=rows * LANES * pairs * 30
        ),
    )(q, near, far, near, far, bias, context, grad, logs, cosine, sine)


class Comm:
    def __init__(self, shape):
        self.rep, self.shard, self.seq = shape["rep"], shape["shard"], shape["seq"]
        assert self.rep == 4 and self.seq == 2
        assert self.shard & (self.shard - 1) == 0
        self.core = lax.axis_index("rep") % 2
        self.x = lax.axis_index("rep") // 2
        self.z = lax.axis_index("shard")
        self.y = lax.axis_index("seq")
        self.bits = self.shard.bit_length() - 1

    def partner(self, array, axis):
        name, size, step = {
            "core": ("rep", self.rep, 1),
            "x": ("rep", self.rep, 2),
            "y": ("seq", self.seq, 1),
        }.get(axis) or ("shard", self.shard, 1 << axis)
        return lax.ppermute(array, name, [(i, i ^ step) for i in range(size)])

    def place(self, axis):
        if axis in ("core", "x", "y"):
            return getattr(self, axis)
        return (self.z >> axis) & 1

    def trade(self, array):
        pairs = [((x * 2 + c) * 2 + 1 - c, (x * 2 + 1 - c) * 2 + c) for x in range(2) for c in range(2)]
        came = lax.ppermute(array, ("rep", "seq"), pairs)
        return jnp.where(self.core == self.y, array, came)

    def merge(self, held, came, axis):
        slot = lax.broadcasted_iota(jnp.int32, (1, 2) + (1,) * (held.ndim - 1), 1)
        return jnp.where(slot == self.place(axis), held[:, None], came[:, None])

    def gather(self, piece, last):
        rows, cols = piece.shape
        held = piece[None]
        for bit in reversed(range(self.bits)):
            merged = self.merge(held, self.partner(held, bit), bit)
            held = merged.reshape(-1, rows, cols)
        if last == "x":
            held = self.merge(held, self.partner(held, "y"), "y").reshape(-1, rows, cols)
            held = self.merge(held, self.partner(held, "x"), "x").reshape(-1, rows, cols)
        else:
            held = self.merge(held, self.partner(held, "x"), "x").reshape(-1, 2 * rows, cols)
            held = self.merge(held, self.partner(held, "y"), "y")
        return held.reshape(-1, cols)

    def halve(self, array, axis, dim):
        mine = lax.dynamic_index_in_dim(array, self.place(axis), dim, keepdims=False)
        other = lax.dynamic_index_in_dim(array, 1 - self.place(axis), dim, keepdims=False)
        came = self.partner(other, axis)
        return (mine.astype(jnp.float32) + came.astype(jnp.float32)).astype(array.dtype)

    def scatter(self, mine, other, first):
        came = self.partner(other, "core")
        held = (mine.astype(jnp.float32) + came.astype(jnp.float32)).astype(jnp.bfloat16)
        cols = held.shape[1]
        rows = held.shape[0] // (self.shard * 4)
        held = held.reshape(self.shard, 2, 2, rows, cols)
        if first == "x":
            held = self.halve(held, "x", 2)
            held = self.halve(held, "y", 1)
        else:
            held = self.halve(held, "y", 1)
            held = self.halve(held, "x", 1)
        for bit in range(self.bits):
            held = self.halve(held.reshape(-1, 2, rows, cols), bit, 1)
        held = self.merge(held.reshape(1, rows, cols), self.partner(held.reshape(1, rows, cols), "x"), "x")
        held = held.reshape(2 * rows, cols)
        return held, self.partner(held, "core")

    def total(self, vector):
        for axis in ["core", "x", "y"] + list(range(self.bits)):
            vector = vector + self.partner(vector, axis)
        return vector

    def relative(self, panels):
        return jnp.where(self.core == 0, panels, panels[..., ::-1, :])


def on_device(shape, tokens, cotangent, pad_mask, image_mask, patch_rows, patch_cols,
              norm1_gain, norm1_bias, w_qkv, query_bias, value_bias, attn_gain, attn_bias,
              w_proj, proj_bias, norm2_gain, norm2_bias, w_gate, gate_bias, w_up, up_bias,
              ffn_gain, ffn_bias, w_down, down_bias):
    comm = Comm(shape)
    images, slot_count, width = tokens.shape
    assert images == 1
    half = width // 2
    rows = slot_count
    hidden_width = w_gate.shape[1]
    panel = -(-hidden_width // (2 * LANES)) * LANES
    score_scale = HEAD ** (-0.5)
    block = w_qkv.shape[0]

    def ff_panels(array):
        pad = [(0, 0)] * (array.ndim - 1) + [(0, 2 * panel - hidden_width)]
        return jnp.pad(array, pad).reshape(array.shape[:-1] + (2, panel))

    def own(array):
        mine = lax.dynamic_index_in_dim(array, comm.core, 1, keepdims=False)
        return lax.dynamic_slice_in_dim(mine, comm.x * (block // 2), block // 2, 0)

    swapped_tokens = comm.trade(tokens.reshape(rows, width))
    packed = jnp.concatenate(
        [pad_mask, patch_rows, patch_cols, jnp.broadcast_to(image_mask[:, None], pad_mask.shape)], 0
    )
    packed = comm.trade(packed)
    live = packed[0]
    packed_far = comm.partner(packed, "core")
    alive = packed[3]
    slots_all = jnp.concatenate([packed, packed_far], 1)
    cosine, sine = angle_tables(slots_all[1], slots_all[2])
    key_bias = jnp.where(slots_all[0] > 0, 0.0, masked_score)[:, None]

    qkv = w_qkv.reshape(block, 3, 2, half)
    value_cut = half // 2
    piece_a = own(jnp.concatenate([qkv[:, 0], qkv[:, 2, :, :value_cut]], -1))
    piece_b = own(jnp.concatenate([qkv[:, 1], qkv[:, 2, :, value_cut:]], -1))
    qv_mine = comm.gather(piece_a, "x")
    kv_mine = comm.gather(piece_b, "y")
    qv_other = comm.partner(qv_mine, "core")
    kv_other = comm.partner(kv_mine, "core")
    proj_panels = w_proj.reshape(block, 2, half)
    gate_piece = own(jnp.concatenate([ff_panels(w_gate), proj_panels], -1))
    gate_mine = comm.gather(gate_piece, "x")
    gate_other = comm.partner(gate_mine, "core")
    up_mine = comm.gather(own(ff_panels(w_up)), "y")
    up_other = comm.partner(up_mine, "core")
    down_mine = comm.gather(own(ff_panels(w_down.T)), "x")
    down_other = comm.partner(down_mine, "core")
    proj_mine, proj_other = gate_mine[:, panel:], gate_other[:, panel:]
    gate_mine, gate_other = gate_mine[:, :panel], gate_other[:, :panel]
    w_proj_all = jnp.where(
        comm.core == 0,
        jnp.concatenate([proj_mine, proj_other], 1),
        jnp.concatenate([proj_other, proj_mine], 1),
    )

    def by_core(vector):
        return comm.relative(vector.reshape(2, -1)).reshape(-1)

    def by_ff(vector):
        return comm.relative(ff_panels(vector)).reshape(-1)

    def from_ff(vector):
        return comm.relative(vector.reshape(2, panel)).reshape(-1)[:hidden_width]

    column = lax.broadcasted_iota(jnp.int32, (2, panel), 0) * panel + lax.broadcasted_iota(
        jnp.int32, (2, panel), 1
    )
    ff_live = comm.relative((column < hidden_width).astype(jnp.float32)).reshape(-1)

    def norm_forward(inputs, gain, bias, count=None, real=None):
        count = count or inputs.shape[-1]
        center = inputs - jnp.sum(inputs, -1, keepdims=True) / count
        if real is not None:
            center = center * real
        inverse = lax.rsqrt(jnp.sum(center * center, -1, keepdims=True) / count + norm_epsilon)
        normal = center * inverse
        return (normal * gain + bias, normal, inverse)

    def norm_backward(grad_out, normal, inverse, gain, count=None):
        count = count or normal.shape[-1]
        scaled = grad_out * gain
        adjusted = (
            scaled
            - jnp.sum(scaled, -1, keepdims=True) / count
            - normal * (jnp.sum(scaled * normal, -1, keepdims=True) / count)
        )
        return (adjusted * inverse, jnp.sum(grad_out * normal, 0), jnp.sum(grad_out, 0))

    inputs = swapped_tokens.astype(jnp.float32)
    normed_one, normal_one, inverse_one = norm_forward(inputs, norm1_gain, norm1_bias)
    normed_one = normed_one.astype(jnp.bfloat16)
    query_bias_rel, value_bias_rel = by_core(query_bias), by_core(value_bias)
    bias_panels = [
        jnp.concatenate([query_bias_rel[p * half : (p + 1) * half], jnp.zeros((half,)), value_bias_rel[p * half : (p + 1) * half]])
        for p in (0, 1)
    ]
    query_mine, near_mine = project(
        normed_one, qv_mine, kv_mine, bias_panels[0], cosine[:rows], sine[:rows]
    )
    query_other, near_other = project(
        normed_one, qv_other, kv_other, bias_panels[1], cosine[:rows], sine[:rows]
    )
    far_mine, far_other = comm.partner(near_other, "core"), comm.partner(near_mine, "core")
    context_mine, logs_mine = attend(query_mine, near_mine, far_mine, key_bias)
    context_other, logs_other = attend(query_other, near_other, far_other, key_bias)
    context = jnp.concatenate([context_mine, context_other], 1)

    def turn(array):
        return jnp.concatenate([array[:, half:], array[:, :half]], 1)

    normed_attn, normal_attn, inverse_attn = norm_forward(context, by_core(attn_gain), by_core(attn_bias))

    def swap_halves(array):
        return jnp.where(comm.core == 0, array, turn(array))

    normed_attn = swap_halves(normed_attn.astype(jnp.bfloat16))
    middle = inputs + product(normed_attn, w_proj_all) + proj_bias
    normed_two, normal_two, inverse_two = norm_forward(middle, norm2_gain, norm2_bias)
    normed_two = normed_two.astype(jnp.bfloat16)
    gate_out = jnp.concatenate([product(normed_two, gate_mine), product(normed_two, gate_other)], 1)
    gate_out = gate_out + by_ff(gate_bias)
    up_out = jnp.concatenate([product(normed_two, up_mine), product(normed_two, up_other)], 1)
    up_out = up_out + by_ff(up_bias)
    sigmoid = jax.nn.sigmoid(gate_out)
    activated = gate_out * sigmoid
    hidden = activated * up_out
    gain_ffn = by_ff(ffn_gain)
    normed_ffn, normal_ffn, inverse_ffn = norm_forward(
        hidden, gain_ffn, by_ff(ffn_bias), hidden_width, ff_live
    )
    normed_ffn = normed_ffn.astype(jnp.bfloat16)
    result = (
        middle
        + back_product(normed_ffn[:, :panel], down_mine)
        + back_product(normed_ffn[:, panel:], down_other)
        + down_bias
    )
    output = comm.trade(result.astype(jnp.bfloat16))

    loss_weight = (live * alive).astype(jnp.float32)
    grad_out = comm.trade(cotangent.reshape(rows, width)).astype(jnp.float32) * loss_weight[:, None]
    grad_down = grad_out.astype(jnp.bfloat16)
    down_bias_grad = jnp.sum(grad_down.astype(jnp.float32), 0)

    def low_outer(left, right):
        return outer_product(left, right).astype(jnp.bfloat16)

    owned_down = comm.scatter(
        low_outer(grad_down, normed_ffn[:, :panel]), low_outer(grad_down, normed_ffn[:, panel:]), "x"
    )
    grad_ffn = jnp.concatenate([product(grad_down, down_mine), product(grad_down, down_other)], 1)
    grad_hidden, ffn_gain_grad, ffn_bias_grad = norm_backward(
        grad_ffn, normal_ffn, inverse_ffn, gain_ffn, hidden_width
    )
    grad_gate = (grad_hidden * up_out * sigmoid * (1.0 + gate_out * (1.0 - sigmoid))).astype(
        jnp.bfloat16
    )
    grad_up = (grad_hidden * activated).astype(jnp.bfloat16)
    gate_bias_grad = jnp.sum(grad_gate.astype(jnp.float32), 0)
    up_bias_grad = jnp.sum(grad_up.astype(jnp.float32), 0)
    owned_gate = comm.scatter(
        low_outer(normed_two, grad_gate[:, :panel]), low_outer(normed_two, grad_gate[:, panel:]), "y"
    )
    owned_up = comm.scatter(
        low_outer(normed_two, grad_up[:, :panel]), low_outer(normed_two, grad_up[:, panel:]), "x"
    )
    grad_normed_two = (
        back_product(grad_gate[:, :panel], gate_mine)
        + back_product(grad_gate[:, panel:], gate_other)
        + back_product(grad_up[:, :panel], up_mine)
        + back_product(grad_up[:, panel:], up_other)
    )
    grad_part_two, norm2_gain_grad, norm2_bias_grad = norm_backward(
        grad_normed_two, normal_two, inverse_two, norm2_gain
    )
    grad_middle = grad_out + grad_part_two
    grad_proj = grad_middle.astype(jnp.bfloat16)
    proj_bias_grad = jnp.sum(grad_proj.astype(jnp.float32), 0)
    grad_proj_rel = swap_halves(grad_proj)
    owned_proj = comm.scatter(
        low_outer(normed_attn, grad_proj_rel[:, :half]),
        low_outer(normed_attn, grad_proj_rel[:, half:]),
        "y",
    )
    grad_context, attn_gain_grad, attn_bias_grad = norm_backward(
        swap_halves(back_product(grad_proj, w_proj_all)), normal_attn, inverse_attn, by_core(attn_gain)
    )
    grad_context = grad_context.astype(jnp.bfloat16)
    split = half // LANES // 2
    grads_qv, grads_kv = [], []
    for p, (query, near, far, ctx, logs) in enumerate(
        (
            (query_mine, near_mine, far_mine, context_mine, logs_mine),
            (query_other, near_other, far_other, context_other, logs_other),
        )
    ):
        pieces = []
        for first in (0, split):
            pieces.append(
                attend_back(
                    query, near, far, key_bias, ctx, grad_context, logs, cosine, sine,
                    first, split, p * 2 * split + first,
                )
            )
        grads_qv.append(pieces)
    folded = []
    for p in (0, 1):
        for piece in (0, 1):
            came = comm.partner(grads_qv[1 - p][piece][2], "core")
            mine = grads_qv[p][piece][1]
            folded.append((mine.astype(jnp.float32) + came.astype(jnp.float32)).astype(jnp.bfloat16))
    grad_qv, grad_kv = [], []
    for p in (0, 1):
        low_part, high_part = folded[2 * p], folded[2 * p + 1]
        grad_qv.append(jnp.concatenate([grads_qv[p][0][0], grads_qv[p][1][0], low_part[1]], 1))
        grad_kv.append(jnp.concatenate([low_part[0], high_part[0], high_part[1]], 1))
    query_bias_grad = jnp.concatenate(
        [jnp.sum(grad_qv[p][:, :half].astype(jnp.float32), 0) for p in (0, 1)]
    )
    value_bias_grad = jnp.concatenate(
        [
            jnp.sum(side[p][:, half:].astype(jnp.float32), 0)
            for p in (0, 1)
            for side in (grad_qv, grad_kv)
        ]
    )
    owned_qv = comm.scatter(low_outer(normed_one, grad_qv[0]), low_outer(normed_one, grad_qv[1]), "x")
    owned_kv = comm.scatter(low_outer(normed_one, grad_kv[0]), low_outer(normed_one, grad_kv[1]), "y")
    grad_normed_one = (
        back_product(grad_qv[0], qv_mine)
        + back_product(grad_qv[1], qv_other)
        + back_product(grad_kv[0], kv_mine)
        + back_product(grad_kv[1], kv_other)
    )
    grad_part_one, norm1_gain_grad, norm1_bias_grad = norm_backward(
        grad_normed_one, normal_one, inverse_one, norm1_gain
    )
    tokens_grad = comm.trade((grad_middle + grad_part_one).astype(jnp.bfloat16)).astype(jnp.float32)

    early = [
        by_core(attn_gain_grad), by_core(attn_bias_grad), proj_bias_grad, norm2_gain_grad,
        norm2_bias_grad, from_ff(gate_bias_grad), from_ff(up_bias_grad), from_ff(ffn_gain_grad),
        from_ff(ffn_bias_grad), down_bias_grad,
    ]
    late = [norm1_gain_grad, norm1_bias_grad, by_core(query_bias_grad), by_core(value_bias_grad)]

    def totals(vectors):
        sizes = [vector.shape[0] for vector in vectors]
        flat = jnp.concatenate(vectors)
        length = -(-flat.shape[0] // 1024) * 1024
        flat = jnp.pad(flat, (0, length - flat.shape[0])).reshape(-1, LANES)
        flat = comm.total(flat).reshape(-1)
        parts, start = [], 0
        for size in sizes:
            parts.append(flat[start : start + size])
            start += size
        return parts

    early, late = totals(early), totals(late)

    def both(pair):
        return jnp.where(
            comm.core == 0, jnp.stack(pair, 1), jnp.stack(pair[::-1], 1)
        ).astype(jnp.float32)

    def from_panels(pair):
        return both(pair).reshape(block, 2 * panel)[:, :hidden_width]

    qv_owned, kv_owned = both(owned_qv), both(owned_kv)
    w_qkv_grad = jnp.concatenate(
        [
            qv_owned[:, :, :half].reshape(block, width),
            kv_owned[:, :, :half].reshape(block, width),
            jnp.concatenate([qv_owned[:, :, half:], kv_owned[:, :, half:]], -1).reshape(block, width),
        ],
        1,
    )
    shape_out = (images, slot_count, width)
    return (
        output.reshape(shape_out),
        tokens_grad.reshape(shape_out),
        late[0],
        late[1],
        w_qkv_grad,
        late[2],
        late[3],
        early[0],
        early[1],
        both(owned_proj).reshape(block, width),
        early[2],
        early[3],
        early[4],
        from_panels(owned_gate),
        early[5],
        from_panels(owned_up),
        early[6],
        early[7],
        early[8],
        from_panels(owned_down).T,
        early[9],
    )


def solution(mesh):
    data, rows, cols, copied = (
        P(("rep", "shard"), "seq", None),
        P(("shard", "seq"), None),
        P(None, ("shard", "seq")),
        P(),
    )
    slots = P(("rep", "shard"), "seq")
    placed = (
        data, data, slots, P(("rep", "shard")), slots, slots, copied, copied, rows, copied, copied,
        copied, copied, rows, copied, copied, copied, rows, copied, rows, copied, copied, copied,
        cols, copied,
    )
    shape = dict(mesh.shape)

    def whole(*arrays):
        return on_device(shape, *arrays)

    return jax.shard_map(
        whole,
        mesh=mesh,
        in_specs=placed,
        out_specs=(
            data, data, copied, copied, rows, copied, copied, copied, copied, rows, copied, copied,
            copied, rows, copied, rows, copied, copied, copied, cols, copied,
        ),
        check_vma=False,
    )
```
